512 devices in a mesh: rng: 8 (over z), az: 64 (over y, x, core).
Axes of the slice: x: 4, y: 8, z: 8, core: 2. Of those that a mesh axis runs over, the one named last changes fastest.
Arguments:
- spectrum: float32 [4096, 2, 32768], P('rng', None, 'az'), may hold values from -9 to 9
- src_block: int32 [256, 32], P('az', 'rng'), may hold values from 0 to 30, as said below
- offsets: int32 [256, 4096], P('az', 'rng'), may hold values from 0 to 127
- tap_weights: float32 [8, 256, 4096], P(None, 'az', 'rng'), may hold values from -2 to 2
Outputs:
- image: float32 [4096, 2, 32768], P(('rng', 'az'))
The draws below stay inside these ranges and needn't reach their ends.
Inputs may be any that keep to these rules, and one draw needn't show every extreme that they name: src_block[g, b] lies between min(b, 30) and min(b + 5, 30); a shift of 5 blocks occurs in every draw.
All inputs are finite; a program needn't handle non-finite values.
Results may differ from the reference program's by a relative error of at most 0.00007.
Values sent between devices are 32-bit elements; how exact they have to be, the bound alone decides.
No kernel may reach another device: no remote copies, remote signals or barrier semaphores. Data moves between devices by JAX's collectives and lax.ppermute only.
A program may use at most 128 MiB of HBM per device.

```python
import jax
import jax.numpy as jnp
from jax import lax

NA = 32768
NRB = 4096
BLOCK = 128
GW = 128
TAPS = 8
SHIFT_B = 5
NG = 256
NOB = 32


def draw_spectrum(key, part):
    position = jnp.arange(NRB, dtype=jnp.float32) / NRB
    noise = jnp.clip(jax.random.normal(key, (NRB, 2, NA), jnp.float32), -5.0, 5.0)
    amplitude = jnp.sqrt(1.0 + 2.0 * position)
    return noise * amplitude[:, None, None]


def draw_src_block(key, part):
    groups = jnp.arange(NG, dtype=jnp.int32)
    blocks = jnp.arange(NOB, dtype=jnp.int32)
    distance = jnp.abs(2 * groups + 1 - NG)
    baseline = SHIFT_B * distance // NG
    jitter = jax.random.randint(key, (NG, NOB), 0, 2).astype(jnp.int32)
    shifted = jnp.minimum(baseline[:, None] + jitter, SHIFT_B)
    shifted = jnp.where(groups[:, None] == 0, SHIFT_B, shifted)
    return jnp.minimum(blocks[None, :] + shifted, NOB - 2).astype(jnp.int32)


def place_ends(result, rng, smallest, largest):
    index_at = [jax.random.randint(jax.random.fold_in(rng, axis), (), 0, length) for axis, length in enumerate(result.shape)]
    widest = result.shape.index(max(result.shape))
    beside = index_at[:widest] + [(index_at[widest] + 1) % result.shape[widest]] + index_at[widest + 1:]
    return result.at[tuple(index_at)].set(smallest).at[tuple(beside)].set(largest)


def block_levels(key, shape, shards, smallest, high):
    loudness, own = 1.0, jax.random.fold_in(key, 6)
    for axis_at, parts in shards:
        heights = jnp.exp(jax.random.uniform(jax.random.fold_in(own, axis_at), (parts,), jnp.float32, smallest / len(shards), high / len(shards)))
        loudness = loudness * jnp.repeat(heights, shape[axis_at] // parts).reshape([-1 if axis == axis_at else 1 for axis in range(len(shape))])
    return loudness


def scatter_about(stream_key, dims, spread, reach, split=(), held_as=jnp.bfloat16):
    level = block_levels(stream_key, dims, split, -0.22, 0.18) if split else 1.0
    entries = jax.random.normal(stream_key, dims, jnp.float32) * spread * level
    return jnp.minimum(jnp.maximum(entries, -reach), reach).astype(held_as)


def setup_inputs(seed: int = 0) -> dict:
    keys = jax.random.split(jax.random.key(seed), 5)
    spectrum = draw_spectrum(jax.random.fold_in(keys[4], 71), 0)
    src_block = draw_src_block(jax.random.fold_in(keys[4], 71), 0)
    offsets = place_ends(jax.random.randint(keys[2], (NG, NRB), 0, BLOCK), jax.random.fold_in(keys[2], 1), 0, BLOCK - 1).astype(jnp.int32)
    tap_weights = scatter_about(keys[3], (TAPS, NG, NRB), 0.35, 2.0, ((1, 64), (2, 8)), jnp.float32)
    return dict(spectrum=spectrum, src_block=src_block, offsets=offsets, tap_weights=tap_weights)


def reference(spectrum, src_block, offsets, tap_weights):
    grouped = spectrum.reshape(NRB, 2, NG, GW).transpose(2, 0, 1, 3).reshape(NG, NRB, 2 * GW)
    src_rows = (src_block[:, :, None] * BLOCK + offsets.reshape(NG, NOB, BLOCK)).reshape(NG, NRB).astype(jnp.int32)

    def pick(table, where):
        return jnp.take(table, where, axis=0)
    remapped = jnp.zeros((NG, NRB, 2 * GW), jnp.float32)
    for tap_index in range(TAPS):
        picked = jax.vmap(pick)(grouped, src_rows + tap_index)
        remapped = remapped + tap_weights[tap_index][:, :, None] * picked
    remapped = remapped.reshape(NG, NRB, 2, GW).transpose(1, 2, 0, 3).reshape(NRB, 2, NA)
    values = jnp.fft.ifft(remapped[:, 0] + 1j * remapped[:, 1], axis=-1)
    band = jnp.stack([jnp.real(values), jnp.imag(values)], axis=1).astype(jnp.float32)
    energy = jnp.sum(band * band)
    scaling = lax.rsqrt(energy / (NRB * NA) + 1e-06)
    return band * scaling
```

```python
import math

import jax
import jax.numpy as jnp
import numpy as np
from jax import lax
from jax.experimental import pallas as pl
from jax.experimental.pallas import tpu as pltpu
from jax.sharding import Mesh
from jax.sharding import PartitionSpec as P

BLOCK = 128
GW = 128
TAPS = 8
HEAD = 136
WIN = 144
AZ = ("az_0", "az_1", "az_2")
RNG_AZ = ("rng", "az_0", "az_1", "az_2")
CHUNKS = ((0,), (1, 3), (2,))
FULL = 63 << 20
ROOM = pltpu.CompilerParams(vmem_limit_bytes=12 << 20)
VMEM = pl.BlockSpec(memory_space=pltpu.VMEM)
SMEM = pl.BlockSpec(memory_space=pltpu.SMEM)


def halves(x):
    high = x.astype(jnp.bfloat16)
    return high, (x - high.astype(jnp.float32)).astype(jnp.bfloat16)


def product(a, b, contract):
    a_high, a_low = a
    b_high, b_low = b

    def times(x, y):
        return lax.dot_general(x, y, (contract, ((), ())), preferred_element_type=jnp.float32)

    return times(a_high, b_high) + times(a_high, b_low) + times(a_low, b_high)


def split_table(table):
    high = table.astype(jnp.bfloat16)
    low = (table - high.astype(np.float64)).astype(jnp.bfloat16)
    return high, low


def first_table(upper):
    a = 2 * np.arange(64) + upper
    ang = (a[:, None] * np.arange(128)[None, :] % 128) * (2 * math.pi / 128)
    cos, sin = np.cos(ang), np.sin(ang)
    return split_table(np.block([[cos, sin], [-sin, cos]]))


def turn_table(half):
    ang = (np.arange(128)[:, None] + 128 * half) * np.arange(128)[None, :] * (2 * math.pi / 32768)
    return np.stack([np.cos(ang), np.sin(ang)]).astype(np.float32)


def second_table(half):
    m = np.arange(128) + 128 * half
    ang = (np.arange(256)[:, None] * m[None] % 256) * (2 * math.pi / 256)
    cos, sin = np.cos(ang) / 32768, np.sin(ang) / 32768
    real = np.concatenate([cos, -sin], axis=1)
    imag = np.concatenate([sin, cos], axis=1)
    return split_table(np.stack([real, imag], axis=1).reshape(512, 256))


def regroup_kernel(x_ref, *out_refs):
    for index, chunk in enumerate(CHUNKS):
        head, rest = out_refs[2 * index], out_refs[2 * index + 1]
        for at, g in enumerate(chunk):
            for c in range(2):
                lanes = pl.ds(128 * c, 128)
                head[at, :, lanes] = x_ref[pl.ds(2 * g + c, HEAD, stride=8), :]
                rest[at, :, lanes] = x_ref[pl.ds(8 * HEAD + 2 * g + c, 512 - HEAD, stride=8), :]


def regroup(flat):
    shapes = []
    for chunk in CHUNKS:
        shapes.append(jax.ShapeDtypeStruct((len(chunk), HEAD, 256), jnp.float32))
        shapes.append(jax.ShapeDtypeStruct((len(chunk), 512 - HEAD, 256), jnp.float32))
    return pl.pallas_call(
        regroup_kernel,
        out_shape=shapes,
        name="regroup",
        compiler_params=ROOM,
    )(flat)


def remap_kernel(src_ref, off_ref, w_ref, a0, b0, a1, b1, a2, before_ref, out_ref, energy_ref, ext):
    count = a0.shape[0]
    energy = before_ref[...]
    ext[1024 + HEAD :, :] = jnp.zeros((ext.shape[0] - 1024 - HEAD, 256), jnp.float32)
    rows = lax.broadcasted_iota(jnp.int32, (WIN, BLOCK), 0)
    for at in range(count):
        ext[0:HEAD, :] = a0[at]
        ext[HEAD:512, :] = b0[at]
        ext[512 : 512 + HEAD, :] = a1[at]
        ext[512 + HEAD : 1024, :] = b1[at]
        ext[1024 : 1024 + HEAD, :] = a2[at]
        for b in range(4):
            start = pl.multiple_of(src_ref[at, b] * BLOCK, BLOCK)
            source = ext[pl.ds(start, WIN), :]
            here = pl.ds(b * BLOCK, BLOCK)
            tap_at = rows - off_ref[at, :, here]
            weights = jnp.zeros((WIN, BLOCK), jnp.float32)
            for t in range(TAPS):
                weights = jnp.where(tap_at == t, w_ref[at, pl.ds(t, 1), here], weights)
            w_high, w_low = halves(weights)
            s_high, s_low = halves(source)
            result = lax.dot_general(
                jnp.concatenate([w_high, w_high, w_low], axis=0),
                jnp.concatenate([s_high, s_low, s_high], axis=0),
                (((0,), (0,)), ((), ())),
                preferred_element_type=jnp.float32,
            )
            for c in range(2):
                part = result[:, 128 * c : 128 * c + 128].reshape(16, 8, 128)
                out_ref[pl.ds(16 * b, 16), at, c] = part
                energy = energy + jnp.sum(part * part, axis=0)
    energy_ref[...] = energy


def remap(src, off, weights, parts, before):
    count = off.shape[0]
    return pl.pallas_call(
        remap_kernel,
        out_shape=[
            jax.ShapeDtypeStruct((64, count, 2, 8, 128), jnp.float32),
            jax.ShapeDtypeStruct((8, 128), jnp.float32),
        ],
        in_specs=[SMEM] + [VMEM] * 8,
        out_specs=[VMEM, VMEM],
        scratch_shapes=[pltpu.VMEM((1024 + WIN, 256), jnp.float32)],
        compiler_params=ROOM,
    )(src, off, weights, *parts, before)


def pack_kernel(x_ref, energy_ref, out_ref):
    total = jnp.full((1, 128), jnp.sum(energy_ref[...]), jnp.float32)
    for a in range(64):
        out_ref[pl.ds(17 * a, 8), :] = x_ref[a, 0, 0]
        out_ref[pl.ds(17 * a + 8, 8), :] = x_ref[a, 0, 1]
        out_ref[pl.ds(17 * a + 16, 1), :] = total


def pack(x, energy):
    return pl.pallas_call(
        pack_kernel,
        out_shape=jax.ShapeDtypeStruct((64 * 17, 128), jnp.float32),
        in_specs=[VMEM, VMEM],
        out_specs=VMEM,
        name="pack",
        compiler_params=ROOM,
    )(x, energy)


def columns(ref, at, stride, rows):
    lanes = []
    for r in rows:
        parts = [ref[pl.ds(16 * at + 8 * c + r, 64, stride=stride), :] for c in range(2)]
        lanes.append(jnp.concatenate(parts, axis=0))
    return halves(jnp.concatenate(lanes, axis=1))


def turned(step, cos, sin):
    lanes = []
    for r in range(step.shape[0] // 128):
        real, imag = step[128 * r : 128 * r + 128, :128], step[128 * r : 128 * r + 128, 128:]
        both = [real * cos - imag * sin, real * sin + imag * cos]
        lanes.append(jnp.concatenate(both, axis=0))
    return halves(jnp.concatenate(lanes, axis=1))


ROWS = ((0,), (0,))
INNER = ((1,), (0,))


def early_kernel(x0, x13, f0h, f0l, f1h, f1l, turn, mh, ml, step_ref, part_ref):
    low = (f0h[...], f0l[...])
    high = (f1h[...], f1l[...])
    step_ref[...] = product(columns(x0, 0, 16, range(8)), low, ROWS)
    for i in range(4):
        rows = (2 * i, 2 * i + 1)
        step = product(columns(x13, 0, 32, rows), low, ROWS)
        step = step + product(columns(x13, 1, 32, rows), high, ROWS)
        data = turned(step, turn[0], turn[1])
        part_ref[:, pl.ds(256 * i, 256)] = product((mh[...], ml[...]), data, INNER)


def early(x0, x13, tables):
    return pl.pallas_call(
        early_kernel,
        out_shape=[
            jax.ShapeDtypeStruct((1024, 256), jnp.float32),
            jax.ShapeDtypeStruct((512, 1024), jnp.float32),
        ],
        in_specs=[VMEM] * 9,
        out_specs=[VMEM, VMEM],
        name="early",
        compiler_params=ROOM,
    )(x0, x13, *tables)


def finish_kernel(x2, step_ref, part_ref, f1h, f1l, turn, mh, ml, out_ref):
    i = pl.program_id(0)
    energy = jnp.sum(x2[pl.ds(16, 64, stride=17), :], axis=0, keepdims=True)
    scale = lax.rsqrt(energy * (1.0 / (32768.0 * 134217728.0)) + 1e-06)
    step = step_ref[...] + product(
        columns(x2, 0, 17, (2 * i, 2 * i + 1)), (f1h[...], f1l[...]), ROWS
    )
    data = turned(step, turn[0], turn[1])
    result = part_ref[...] + product((mh[...], ml[...]), data, INNER)
    for at in range(2):
        out_ref[at] = result[:, 128 * at : 128 * at + 128] * scale


def finish(x2, step, part, tables):
    def whole(shape):
        return pl.BlockSpec(shape, lambda i: (0,) * len(shape))

    return pl.pallas_call(
        finish_kernel,
        out_shape=jax.ShapeDtypeStruct((8, 512, 128), jnp.float32),
        grid=(4,),
        in_specs=[
            whole((1088, 128)),
            pl.BlockSpec((256, 256), lambda i: (i, 0)),
            pl.BlockSpec((512, 256), lambda i: (0, i)),
        ]
        + [whole(t.shape) for t in tables],
        out_specs=pl.BlockSpec((2, 512, 128), lambda i: (i, 0, 0)),
        name="finish",
        compiler_params=pltpu.CompilerParams(vmem_limit_bytes=FULL),
    )(x2, step, part, *tables)


def steps(spectrum, src_block, offsets, tap_weights):
    position = lax.axis_index("rng")
    size = lax.axis_size("rng")
    down = [(i, i - 1) for i in range(1, size)]
    flat = spectrum.reshape(512, 2, 4, GW).transpose(0, 2, 1, 3).reshape(4096, GW)
    local = regroup(flat)
    src = jnp.clip(src_block - 4 * position, 0, 8)
    off = offsets.reshape(4, 1, 512)
    weights = tap_weights.transpose(1, 0, 2)

    def pull(x):
        return lax.ppermute(x, "rng", down)

    def swap(x):
        return lax.all_to_all(x, AZ, split_axis=0, concat_axis=0, tiled=True)

    energy = jnp.zeros((8, 128), jnp.float32)
    moved = []
    for i, chunk in enumerate(CHUNKS):
        near, far = local[2 * i], local[2 * i + 1]
        near_up = pull(near)
        far_up = pull(far)
        near_up_up = pull(near_up)

        def of_chunk(x):
            return jnp.concatenate([x[g : g + 1] for g in chunk], axis=0)

        out, energy = remap(
            of_chunk(src),
            of_chunk(off),
            of_chunk(weights),
            (near, far, near_up, far_up, near_up_up),
            energy,
        )
        moved.append(out)
    got0 = swap(moved[0]).reshape(1024, 128)
    got1 = swap(moved[1]).reshape(2048, 128)
    energy = lax.psum(energy, "rng")
    packed = pack(moved[2], energy).reshape(64, 1, 17 * 128)
    got2 = swap(packed).reshape(1088, 128)
    f0, f1 = first_table(0), first_table(1)
    step, part = early(got0, got1, (*f0, *f1, turn_table(1), *second_table(1)))
    out = finish(got2, step, part, (*f1, turn_table(0), *second_table(0)))
    return out.reshape(8, 256, 2, 128).transpose(0, 2, 1, 3).reshape(8, 2, 32768)


def solution(mesh):
    torus = Mesh(mesh.devices.reshape(mesh.shape["rng"], 8, 4, 2), RNG_AZ)
    placed = (P("rng", None, AZ), P(AZ, "rng"), P(AZ, "rng"), P(None, AZ, "rng"))
    return jax.shard_map(
        steps, mesh=torus, in_specs=placed, out_specs=P(RNG_AZ, None, None), check_vma=False
    )
```

```python
import math

import jax
import jax.numpy as jnp
import numpy as np
from jax import lax
from jax.experimental import pallas as pl
from jax.experimental.pallas import tpu as pltpu
from jax.sharding import Mesh
from jax.sharding import PartitionSpec as P

BLOCK = 128
GW = 128
TAPS = 8
HEAD = 136
WIN = 144
AZ = ("az_0", "az_1", "az_2")
RNG_AZ = ("rng", "az_0", "az_1", "az_2")
CHUNKS = (((3, 0), (3, 1)), ((1, 0), (1, 1), (0, 0)), ((0, 1), (2, 0), (2, 1)))
FULL = 63 << 20
ROOM = pltpu.CompilerParams(vmem_limit_bytes=12 << 20)
VMEM = pl.BlockSpec(memory_space=pltpu.VMEM)
ANY = pl.BlockSpec(memory_space=pl.ANY)
SMEM = pl.BlockSpec(memory_space=pltpu.SMEM)


ROWS = ((0,), (0,))
INNER = ((1,), (0,))


def halves(x):
    high = x.astype(jnp.bfloat16)
    return high, (x - high.astype(jnp.float32)).astype(jnp.bfloat16)


def product(a, b, contract):
    ((at,), (bt,)) = contract
    left = jnp.concatenate([a[0], a[0], a[1]], axis=at)
    right = jnp.concatenate([b[0], b[1], b[0]], axis=bt)
    return lax.dot_general(left, right, (contract, ((), ())), preferred_element_type=jnp.float32)


def split_table(table):
    high = np.asarray(table).astype(jnp.bfloat16)
    low = (table - high.astype(np.float64)).astype(jnp.bfloat16)
    return high, low


def first_table(upper):
    a = 2 * np.arange(64) + upper
    ang = (a[:, None] * np.arange(128)[None, :] % 128) * (2 * math.pi / 128)
    cos, sin = np.cos(ang), np.sin(ang)
    return split_table(np.block([[cos, sin], [-sin, cos]]))


def turn_table(half):
    ang = (np.arange(128)[:, None] + 128 * half) * np.arange(128)[None, :] * (2 * math.pi / 32768)
    return np.stack([np.cos(ang), np.sin(ang)]).astype(np.float32)


def second_table(half):
    m = np.arange(128) + 128 * half
    ang = (np.arange(256)[:, None] * m[None] % 256) * (2 * math.pi / 256)
    cos, sin = np.cos(ang) / 32768, np.sin(ang) / 32768
    real = np.concatenate([cos, -sin], axis=1)
    imag = np.concatenate([sin, cos], axis=1)
    return split_table(np.stack([real, imag], axis=1).reshape(512, 256))


def groups_of(chunk):
    return tuple(dict.fromkeys(g for g, _ in chunk))


def regroup_kernel(x_hbm, *refs):
    out_refs, x_ref, sems = refs[:-2], refs[-2], refs[-1]
    copies = []
    for n in range(4):
        rows = pl.ds(1024 * n, 1024)
        copies.append(pltpu.make_async_copy(x_hbm.at[rows], x_ref.at[rows], sems.at[n]))
        copies[n].start()
    for n in range(4):
        copies[n].wait()
        for index, chunk in enumerate(CHUNKS):
            head, rest = out_refs[2 * index], out_refs[2 * index + 1]
            for at, (g, c) in enumerate(chunk):
                lanes = pl.ds(128 * at, 128)

                def take(first, count):
                    return x_ref[pl.ds(8 * first + 2 * g + c, count, stride=8), :]

                if n == 0:
                    head[0:128, lanes] = take(0, 128)
                elif n == 1:
                    head[128:HEAD, lanes] = take(128, HEAD - 128)
                    rest[0 : 256 - HEAD, lanes] = take(HEAD, 256 - HEAD)
                else:
                    start = 128 * n - HEAD
                    rest[start : start + 128, lanes] = take(128 * n, 128)


def regroup(flat):
    shapes = []
    for chunk in CHUNKS:
        shapes.append(jax.ShapeDtypeStruct((HEAD, 128 * len(chunk)), jnp.float32))
        shapes.append(jax.ShapeDtypeStruct((512 - HEAD, 128 * len(chunk)), jnp.float32))
    return pl.pallas_call(
        regroup_kernel,
        out_shape=shapes,
        in_specs=[pl.BlockSpec(memory_space=pltpu.HBM)],
        out_specs=[VMEM] * len(shapes),
        scratch_shapes=[pltpu.VMEM((4096, 128), jnp.float32), pltpu.SemaphoreType.DMA((4,))],
        name="regroup",
        compiler_params=ROOM,
    )(flat)


def remap_kernel(chunk, src_ref, off_ref, w_ref, a0, b0, a1, b1, a2, before_ref, out_ref, energy_ref, ext):
    energy = before_ref[...]
    ext[0:HEAD, :] = a0[...]
    ext[HEAD:512, :] = b0[...]
    ext[512 : 512 + HEAD, :] = a1[...]
    ext[512 + HEAD : 1024, :] = b1[...]
    ext[1024 : 1024 + HEAD, :] = a2[...]
    ext[1024 + HEAD :, :] = jnp.zeros((WIN - HEAD, ext.shape[1]), jnp.float32)
    rows = lax.broadcasted_iota(jnp.int32, (WIN, BLOCK), 0)
    for which, group in enumerate(groups_of(chunk)):
        units = [at for at, (g, _) in enumerate(chunk) if g == group]
        lanes = slice(128 * units[0], 128 * units[-1] + 128)
        for b in range(4):
            start = pl.multiple_of(src_ref[which, b] * BLOCK, BLOCK)
            source = ext[pl.ds(start, WIN), lanes]
            here = pl.ds(b * BLOCK, BLOCK)
            tap_at = rows - off_ref[which, :, here]
            weights = jnp.zeros((WIN, BLOCK), jnp.float32)
            for t in range(TAPS):
                weights = jnp.where(tap_at == t, w_ref[which, pl.ds(t, 1), here], weights)
            result = product(halves(weights), halves(source), ROWS)
            for n, at in enumerate(units):
                part = result[:, 128 * n : 128 * n + 128].reshape(16, 8, 128)
                out_ref[pl.ds(16 * b, 16), at] = part
                energy = energy + jnp.sum(part * part, axis=0)
    energy_ref[...] = energy


def remap(chunk, src, off, weights, parts, before):
    return pl.pallas_call(
        lambda *refs: remap_kernel(chunk, *refs),
        out_shape=[
            jax.ShapeDtypeStruct((64, len(chunk), 8, 128), jnp.float32),
            jax.ShapeDtypeStruct((8, 128), jnp.float32),
        ],
        in_specs=[SMEM] + [VMEM] * 8,
        out_specs=[VMEM, VMEM],
        scratch_shapes=[pltpu.VMEM((1024 + WIN, 128 * len(chunk)), jnp.float32)],
        compiler_params=ROOM,
    )(src, off, weights, *parts, before)


def pack_kernel(x_ref, energy_ref, out_ref):
    count = x_ref.shape[1]
    rows = 8 * count + 1
    total = jnp.full((1, 128), jnp.sum(energy_ref[...]), jnp.float32)
    for a in range(64):
        for at in range(count):
            out_ref[pl.ds(rows * a + 8 * at, 8), :] = x_ref[a, at]
        out_ref[pl.ds(rows * a + rows - 1, 1), :] = total


def pack(x, energy):
    return pl.pallas_call(
        pack_kernel,
        out_shape=jax.ShapeDtypeStruct((64 * (8 * x.shape[1] + 1), 128), jnp.float32),
        in_specs=[VMEM, VMEM],
        out_specs=VMEM,
        name="pack",
        compiler_params=ROOM,
    )(x, energy)


def columns(pieces, rows):
    lanes = []
    for r in rows:
        parts = [ref[pl.ds(8 * at + r, 64, stride=ref.shape[0] // 64), :] for ref, at in pieces]
        lanes.append(jnp.concatenate(parts, axis=0))
    return halves(jnp.concatenate(lanes, axis=1))


def turned(step, cos, sin):
    lanes = []
    for r in range(step.shape[0] // 128):
        real, imag = step[128 * r : 128 * r + 128, :128], step[128 * r : 128 * r + 128, 128:]
        both = [real * cos - imag * sin, real * sin + imag * cos]
        lanes.append(jnp.concatenate(both, axis=0))
    return halves(jnp.concatenate(lanes, axis=1))


def early_kernel(x0, x1, fah, fal, fbh, fbl, turn, mh, ml, step_ref, part_ref):
    step_ref[...] = product(columns([(x1, 2)], range(8)), (fah[...], fal[...]), ROWS)
    for i in range(4):
        pieces = [(x1, 0), (x1, 1), (x0, 0), (x0, 1)]
        step = product(columns(pieces, (2 * i, 2 * i + 1)), (fbh[...], fbl[...]), ROWS)
        data = turned(step, turn[0], turn[1])
        part_ref[:, pl.ds(256 * i, 256)] = product((mh[...], ml[...]), data, INNER)


def early(x0, x1, tables):
    return pl.pallas_call(
        early_kernel,
        out_shape=[
            jax.ShapeDtypeStruct((1024, 256), jnp.float32),
            jax.ShapeDtypeStruct((512, 1024), jnp.float32),
        ],
        in_specs=[VMEM] * 9,
        out_specs=[VMEM, VMEM],
        name="early",
        compiler_params=ROOM,
    )(x0, x1, *tables)


def finish_kernel(*refs):
    sources, out_hbm, held = refs[:8], refs[8], refs[9:17]
    out_ref, load_sems, store_sems = refs[17:]
    x2, fh, fl, step_ref, turn, mh, ml, part_ref = held
    loads = [
        pltpu.make_async_copy(source, here, load_sems.at[n])
        for n, (source, here) in enumerate(zip(sources[:7], held[:7]))
    ]
    for i in range(4):
        lanes = pl.ds(256 * i, 256)
        loads.append(
            pltpu.make_async_copy(
                sources[7].at[:, lanes], part_ref.at[:, lanes], load_sems.at[7 + i]
            )
        )
    for copy in loads:
        copy.start()
    for copy in loads[:5]:
        copy.wait()
    energy = jnp.sum(x2[pl.ds(24, 64, stride=25), :], axis=0, keepdims=True)
    scale = lax.rsqrt(energy * (1.0 / (32768.0 * 134217728.0)) + 1e-06)
    pieces = [(x2, 0), (x2, 1), (x2, 2)]
    stores = []
    for i in range(4):
        moved = product(columns(pieces, (2 * i, 2 * i + 1)), (fh[...], fl[...]), ROWS)
        data = turned(step_ref[pl.ds(256 * i, 256), :] + moved, turn[0], turn[1])
        if i == 0:
            loads[5].wait()
            loads[6].wait()
        result = product((mh[...], ml[...]), data, INNER)
        loads[7 + i].wait()
        result = result + part_ref[:, pl.ds(256 * i, 256)]
        for at in range(2):
            out_ref[2 * i + at] = result[:, 128 * at : 128 * at + 128] * scale
        pair = pl.ds(2 * i, 2)
        stores.append(pltpu.make_async_copy(out_ref.at[pair], out_hbm.at[pair], store_sems.at[i]))
        stores[i].start()
    for copy in stores:
        copy.wait()


def finish(x2, step, part, tables):
    fh, fl, turn, mh, ml = tables
    operands = (x2, fh, fl, step, turn, mh, ml, part)
    return pl.pallas_call(
        finish_kernel,
        out_shape=jax.ShapeDtypeStruct((8, 512, 128), jnp.float32),
        in_specs=[ANY] * 8,
        out_specs=ANY,
        scratch_shapes=[pltpu.VMEM(x.shape, x.dtype) for x in operands]
        + [
            pltpu.VMEM((8, 512, 128), jnp.float32),
            pltpu.SemaphoreType.DMA((11,)),
            pltpu.SemaphoreType.DMA((4,)),
        ],
        name="finish",
        compiler_params=pltpu.CompilerParams(vmem_limit_bytes=FULL),
    )(*operands)


def steps(spectrum, src_block, offsets, tap_weights):
    position = lax.axis_index("rng")
    size = lax.axis_size("rng")
    down = [(i, i - 1) for i in range(1, size)]
    flat = spectrum.reshape(512, 2, 4, GW).transpose(0, 2, 1, 3).reshape(4096, GW)
    local = regroup(flat)
    src = jnp.clip(src_block - 4 * position, 0, 8)
    off = offsets.reshape(4, 1, 512)
    weights = tap_weights.transpose(1, 0, 2)

    def pull(x):
        return lax.ppermute(x, "rng", down)

    def swap(x):
        return lax.all_to_all(x, AZ, split_axis=0, concat_axis=0, tiled=True)

    energy = jnp.zeros((8, 128), jnp.float32)
    moved = []
    for i, chunk in enumerate(CHUNKS):
        near, far = local[2 * i], local[2 * i + 1]
        near_up = pull(near)
        far_up = pull(far)
        near_up_up = pull(near_up)

        def of_chunk(x):
            return jnp.concatenate([x[g : g + 1] for g in groups_of(chunk)], axis=0)

        out, energy = remap(
            chunk,
            of_chunk(src),
            of_chunk(off),
            of_chunk(weights),
            (near, far, near_up, far_up, near_up_up),
            energy,
        )
        moved.append(out)
    got0 = swap(moved[0]).reshape(-1, 128)
    got1 = swap(moved[1]).reshape(-1, 128)
    energy = lax.psum(energy, "rng")
    packed = pack(moved[2], energy)
    got2 = swap(packed.reshape(64, 1, -1)).reshape(packed.shape)
    lower, upper = first_table(0), first_table(1)
    first = [x[:64] for x in lower]
    second = [np.concatenate([x, y]) for x, y in zip(lower, upper)]
    third = [np.concatenate([x[64:], y]) for x, y in zip(lower, upper)]
    step, part = early(got0, got1, (*first, *second, turn_table(1), *second_table(1)))
    out = finish(got2, step, part, (*third, turn_table(0), *second_table(0)))
    return out.reshape(8, 256, 2, 128).transpose(0, 2, 1, 3).reshape(8, 2, 32768)


def solution(mesh):
    torus = Mesh(mesh.devices.reshape(mesh.shape["rng"], 8, 4, 2), RNG_AZ)
    placed = (P("rng", None, AZ), P(AZ, "rng"), P(AZ, "rng"), P(None, AZ, "rng"))
    return jax.shard_map(
        steps, mesh=torus, in_specs=placed, out_specs=P(RNG_AZ, None, None), check_vma=False
    )
```

```python
import math

import jax
import jax.numpy as jnp
import numpy as np
from jax import lax
from jax.experimental import pallas as pl
from jax.experimental.pallas import tpu as pltpu
from jax.sharding import Mesh
from jax.sharding import PartitionSpec as P

BLOCK = 128
GW = 128
TAPS = 8
HEAD = 136
WIN = 144
AZ = ("az_0", "az_1", "az_2")
RNG_AZ = ("rng", "az_0", "az_1", "az_2")
CHUNKS = ((0,), (1, 3), (2,))
FULL = 63 << 20
ROOM = pltpu.CompilerParams(vmem_limit_bytes=12 << 20)
VMEM = pl.BlockSpec(memory_space=pltpu.VMEM)
ANY = pl.BlockSpec(memory_space=pl.ANY)
SMEM = pl.BlockSpec(memory_space=pltpu.SMEM)


def halves(x):
    high = x.astype(jnp.bfloat16)
    return high, (x - high.astype(jnp.float32)).astype(jnp.bfloat16)


def product(a, b, contract):
    ((at,), (bt,)) = contract
    left = jnp.concatenate([a[0], a[0], a[1]], axis=at)
    right = jnp.concatenate([b[0], b[1], b[0]], axis=bt)
    return lax.dot_general(left, right, (contract, ((), ())), preferred_element_type=jnp.float32)


def split_table(table):
    high = table.astype(jnp.bfloat16)
    low = (table - high.astype(np.float64)).astype(jnp.bfloat16)
    return high, low


def first_table(upper):
    a = 2 * np.arange(64) + upper
    ang = (a[:, None] * np.arange(128)[None, :] % 128) * (2 * math.pi / 128)
    cos, sin = np.cos(ang), np.sin(ang)
    return split_table(np.block([[cos, sin], [-sin, cos]]))


def turn_table(half):
    ang = (np.arange(128)[:, None] + 128 * half) * np.arange(128)[None, :] * (2 * math.pi / 32768)
    return np.stack([np.cos(ang), np.sin(ang)]).astype(np.float32)


def second_table(half):
    m = np.arange(128) + 128 * half
    ang = (np.arange(256)[:, None] * m[None] % 256) * (2 * math.pi / 256)
    cos, sin = np.cos(ang) / 32768, np.sin(ang) / 32768
    real = np.concatenate([cos, -sin], axis=1)
    imag = np.concatenate([sin, cos], axis=1)
    return split_table(np.stack([real, imag], axis=1).reshape(512, 256))


def regroup_kernel(x_hbm, *refs):
    out_refs, x_ref, sems = refs[:-2], refs[-2], refs[-1]
    copies = []
    for n in range(4):
        rows = pl.ds(1024 * n, 1024)
        copies.append(pltpu.make_async_copy(x_hbm.at[rows], x_ref.at[rows], sems.at[n]))
        copies[n].start()
    for n in range(4):
        copies[n].wait()
        for index, chunk in enumerate(CHUNKS):
            head, rest = out_refs[2 * index], out_refs[2 * index + 1]
            for at, g in enumerate(chunk):
                for c in range(2):
                    lanes = pl.ds(128 * c, 128)

                    def take(first, count):
                        return x_ref[pl.ds(8 * first + 2 * g + c, count, stride=8), :]

                    if n == 0:
                        head[at, 0:128, lanes] = take(0, 128)
                    elif n == 1:
                        head[at, 128:HEAD, lanes] = take(128, HEAD - 128)
                        rest[at, 0 : 256 - HEAD, lanes] = take(HEAD, 256 - HEAD)
                    else:
                        start = 128 * n - HEAD
                        rest[at, start : start + 128, lanes] = take(128 * n, 128)


def regroup(flat):
    shapes = []
    for chunk in CHUNKS:
        shapes.append(jax.ShapeDtypeStruct((len(chunk), HEAD, 256), jnp.float32))
        shapes.append(jax.ShapeDtypeStruct((len(chunk), 512 - HEAD, 256), jnp.float32))
    return pl.pallas_call(
        regroup_kernel,
        out_shape=shapes,
        in_specs=[pl.BlockSpec(memory_space=pltpu.HBM)],
        out_specs=[VMEM] * len(shapes),
        scratch_shapes=[pltpu.VMEM((4096, 128), jnp.float32), pltpu.SemaphoreType.DMA((4,))],
        name="regroup",
        compiler_params=ROOM,
    )(flat)


def remap_kernel(src_ref, off_ref, w_ref, a0, b0, a1, b1, a2, before_ref, out_ref, energy_ref, ext):
    count = a0.shape[0]
    energy = before_ref[...]
    ext[1024 + HEAD :, :] = jnp.zeros((ext.shape[0] - 1024 - HEAD, 256), jnp.float32)
    rows = lax.broadcasted_iota(jnp.int32, (WIN, BLOCK), 0)
    for at in range(count):
        ext[0:HEAD, :] = a0[at]
        ext[HEAD:512, :] = b0[at]
        ext[512 : 512 + HEAD, :] = a1[at]
        ext[512 + HEAD : 1024, :] = b1[at]
        ext[1024 : 1024 + HEAD, :] = a2[at]
        for b in range(4):
            start = pl.multiple_of(src_ref[at, b] * BLOCK, BLOCK)
            source = ext[pl.ds(start, WIN), :]
            here = pl.ds(b * BLOCK, BLOCK)
            tap_at = rows - off_ref[at, :, here]
            weights = jnp.zeros((WIN, BLOCK), jnp.float32)
            for t in range(TAPS):
                weights = jnp.where(tap_at == t, w_ref[at, pl.ds(t, 1), here], weights)
            w_high, w_low = halves(weights)
            s_high, s_low = halves(source)
            result = lax.dot_general(
                jnp.concatenate([w_high, w_high, w_low], axis=0),
                jnp.concatenate([s_high, s_low, s_high], axis=0),
                (((0,), (0,)), ((), ())),
                preferred_element_type=jnp.float32,
            )
            for c in range(2):
                part = result[:, 128 * c : 128 * c + 128].reshape(16, 8, 128)
                out_ref[pl.ds(16 * b, 16), at, c] = part
                energy = energy + jnp.sum(part * part, axis=0)
    energy_ref[...] = energy


def remap(src, off, weights, parts, before):
    count = off.shape[0]
    return pl.pallas_call(
        remap_kernel,
        out_shape=[
            jax.ShapeDtypeStruct((64, count, 2, 8, 128), jnp.float32),
            jax.ShapeDtypeStruct((8, 128), jnp.float32),
        ],
        in_specs=[SMEM] + [VMEM] * 8,
        out_specs=[VMEM, VMEM],
        scratch_shapes=[pltpu.VMEM((1024 + WIN, 256), jnp.float32)],
        compiler_params=ROOM,
    )(src, off, weights, *parts, before)


def pack_kernel(x_ref, energy_ref, out_ref):
    total = jnp.full((1, 128), jnp.sum(energy_ref[...]), jnp.float32)
    for a in range(64):
        out_ref[pl.ds(17 * a, 8), :] = x_ref[a, 0, 0]
        out_ref[pl.ds(17 * a + 8, 8), :] = x_ref[a, 0, 1]
        out_ref[pl.ds(17 * a + 16, 1), :] = total


def pack(x, energy):
    return pl.pallas_call(
        pack_kernel,
        out_shape=jax.ShapeDtypeStruct((64 * 17, 128), jnp.float32),
        in_specs=[VMEM, VMEM],
        out_specs=VMEM,
        name="pack",
        compiler_params=ROOM,
    )(x, energy)


def columns(ref, at, stride, rows):
    lanes = []
    for r in rows:
        parts = [ref[pl.ds(16 * at + 8 * c + r, 64, stride=stride), :] for c in range(2)]
        lanes.append(jnp.concatenate(parts, axis=0))
    return halves(jnp.concatenate(lanes, axis=1))


def turned(step, cos, sin):
    lanes = []
    for r in range(step.shape[0] // 128):
        real, imag = step[128 * r : 128 * r + 128, :128], step[128 * r : 128 * r + 128, 128:]
        both = [real * cos - imag * sin, real * sin + imag * cos]
        lanes.append(jnp.concatenate(both, axis=0))
    return halves(jnp.concatenate(lanes, axis=1))


ROWS = ((0,), (0,))
INNER = ((1,), (0,))


def early_kernel(x0, x13, f0h, f0l, f1h, f1l, turn, mh, ml, step_ref, part_ref):
    low = (f0h[...], f0l[...])
    high = (f1h[...], f1l[...])
    step_ref[...] = product(columns(x0, 0, 16, range(8)), low, ROWS)
    for i in range(4):
        rows = (2 * i, 2 * i + 1)
        step = product(columns(x13, 0, 32, rows), low, ROWS)
        step = step + product(columns(x13, 1, 32, rows), high, ROWS)
        data = turned(step, turn[0], turn[1])
        part_ref[:, pl.ds(256 * i, 256)] = product((mh[...], ml[...]), data, INNER)


def early(x0, x13, tables):
    return pl.pallas_call(
        early_kernel,
        out_shape=[
            jax.ShapeDtypeStruct((1024, 256), jnp.float32),
            jax.ShapeDtypeStruct((512, 1024), jnp.float32),
        ],
        in_specs=[VMEM] * 9,
        out_specs=[VMEM, VMEM],
        name="early",
        compiler_params=ROOM,
    )(x0, x13, *tables)


def finish_kernel(*refs):
    sources, out_hbm, held = refs[:8], refs[8], refs[9:17]
    out_ref, load_sems, store_sems = refs[17:]
    x2, fh, fl, turn, mh, ml, step_ref, part_ref = held
    pairs = [(source, here) for source, here in zip(sources[:6], held[:6])]
    for i in range(4):
        rows = pl.ds(256 * i, 256)
        pairs.append((sources[6].at[rows], step_ref.at[rows]))
    for i in range(4):
        lanes = pl.ds(256 * i, 256)
        pairs.append((sources[7].at[:, lanes], part_ref.at[:, lanes]))
    loads = [
        pltpu.make_async_copy(source, here, load_sems.at[n])
        for n, (source, here) in enumerate(pairs)
    ]
    for n in (0, 1, 2, 6, 3, 4, 5, 10, 7, 11, 8, 12, 9, 13):
        loads[n].start()
    for copy in loads[:4]:
        copy.wait()
    energy = jnp.sum(x2[pl.ds(16, 64, stride=17), :], axis=0, keepdims=True)
    scale = lax.rsqrt(energy * (1.0 / (32768.0 * 134217728.0)) + 1e-06)
    stores = []
    for i in range(4):
        pair = (2 * i, 2 * i + 1)
        moved = product(columns(x2, 0, 17, pair), (fh[...], fl[...]), ROWS)
        loads[6 + i].wait()
        data = turned(step_ref[pl.ds(256 * i, 256), :] + moved, turn[0], turn[1])
        if i == 0:
            loads[4].wait()
            loads[5].wait()
        result = product((mh[...], ml[...]), data, INNER)
        loads[10 + i].wait()
        result = result + part_ref[:, pl.ds(256 * i, 256)]
        for at in range(2):
            out_ref[2 * i + at] = result[:, 128 * at : 128 * at + 128] * scale
        both = pl.ds(2 * i, 2)
        stores.append(pltpu.make_async_copy(out_ref.at[both], out_hbm.at[both], store_sems.at[i]))
        stores[i].start()
    for copy in stores:
        copy.wait()


def finish(x2, step, part, tables):
    fh, fl, turn, mh, ml = tables
    operands = (x2, fh, fl, turn, mh, ml, step, part)
    return pl.pallas_call(
        finish_kernel,
        out_shape=jax.ShapeDtypeStruct((8, 512, 128), jnp.float32),
        in_specs=[ANY] * 8,
        out_specs=ANY,
        scratch_shapes=[pltpu.VMEM(x.shape, x.dtype) for x in operands]
        + [
            pltpu.VMEM((8, 512, 128), jnp.float32),
            pltpu.SemaphoreType.DMA((14,)),
            pltpu.SemaphoreType.DMA((4,)),
        ],
        name="finish",
        compiler_params=pltpu.CompilerParams(vmem_limit_bytes=FULL),
    )(*operands)


def steps(spectrum, src_block, offsets, tap_weights):
    position = lax.axis_index("rng")
    size = lax.axis_size("rng")
    down = [(i, i - 1) for i in range(1, size)]
    flat = spectrum.reshape(512, 2, 4, GW).transpose(0, 2, 1, 3).reshape(4096, GW)
    local = regroup(flat)
    src = jnp.clip(src_block - 4 * position, 0, 8)
    off = offsets.reshape(4, 1, 512)
    weights = tap_weights.transpose(1, 0, 2)

    def pull(x):
        return lax.ppermute(x, "rng", down)

    def swap(x):
        return lax.all_to_all(x, AZ, split_axis=0, concat_axis=0, tiled=True)

    energy = jnp.zeros((8, 128), jnp.float32)
    moved = []
    for i, chunk in enumerate(CHUNKS):
        near, far = local[2 * i], local[2 * i + 1]
        near_up = pull(near)
        far_up = pull(far)
        near_up_up = pull(near_up)

        def of_chunk(x):
            return jnp.concatenate([x[g : g + 1] for g in chunk], axis=0)

        out, energy = remap(
            of_chunk(src),
            of_chunk(off),
            of_chunk(weights),
            (near, far, near_up, far_up, near_up_up),
            energy,
        )
        moved.append(out)
    got0 = swap(moved[0]).reshape(1024, 128)
    got1 = swap(moved[1]).reshape(2048, 128)
    energy = lax.psum(energy, "rng")
    packed = pack(moved[2], energy).reshape(64, 1, 17 * 128)
    got2 = swap(packed).reshape(1088, 128)
    f0, f1 = first_table(0), first_table(1)
    step, part = early(got0, got1, (*f0, *f1, turn_table(1), *second_table(1)))
    out = finish(got2, step, part, (*f1, turn_table(0), *second_table(0)))
    return out.reshape(8, 256, 2, 128).transpose(0, 2, 1, 3).reshape(8, 2, 32768)


def solution(mesh):
    torus = Mesh(mesh.devices.reshape(mesh.shape["rng"], 8, 4, 2), RNG_AZ)
    placed = (P("rng", None, AZ), P(AZ, "rng"), P(AZ, "rng"), P(None, AZ, "rng"))
    return jax.shard_map(
        steps, mesh=torus, in_specs=placed, out_specs=P(RNG_AZ, None, None), check_vma=False
    )
```

```python
import math

import jax
import jax.numpy as jnp
import numpy as np
from jax import lax
from jax.experimental import pallas as pl
from jax.experimental.pallas import tpu as pltpu
from jax.sharding import Mesh
from jax.sharding import PartitionSpec as P

BLOCK = 128
GW = 128
TAPS = 8
HEAD = 136
WIN = 144
AZ = ("az_0", "az_1", "az_2")
RNG_AZ = ("rng", "az_0", "az_1", "az_2")
CHUNKS = ((0,), (1, 3), (2,))
FULL = 63 << 20
ROOM = pltpu.CompilerParams(vmem_limit_bytes=12 << 20)
VMEM = pl.BlockSpec(memory_space=pltpu.VMEM)
ANY = pl.BlockSpec(memory_space=pl.ANY)
SMEM = pl.BlockSpec(memory_space=pltpu.SMEM)


def halves(x):
    high = x.astype(jnp.bfloat16)
    return high, (x - high.astype(jnp.float32)).astype(jnp.bfloat16)


def product(a, b, contract):
    ((at,), (bt,)) = contract
    left = jnp.concatenate([a[0], a[0], a[1]], axis=at)
    right = jnp.concatenate([b[0], b[1], b[0]], axis=bt)
    return lax.dot_general(left, right, (contract, ((), ())), preferred_element_type=jnp.float32)


def split_table(table):
    high = table.astype(jnp.bfloat16)
    low = (table - high.astype(np.float64)).astype(jnp.bfloat16)
    return high, low


def first_table(upper):
    a = 2 * np.arange(64) + upper
    ang = (a[:, None] * np.arange(128)[None, :] % 128) * (2 * math.pi / 128)
    cos, sin = np.cos(ang), np.sin(ang)
    return split_table(np.block([[cos, sin], [-sin, cos]]))


def turn_table(half):
    ang = (np.arange(128)[:, None] + 128 * half) * np.arange(128)[None, :] * (2 * math.pi / 32768)
    return np.stack([np.cos(ang), np.sin(ang)]).astype(np.float32)


def second_table(half):
    m = np.arange(128) + 128 * half
    ang = (np.arange(256)[:, None] * m[None] % 256) * (2 * math.pi / 256)
    cos, sin = np.cos(ang) / 32768, np.sin(ang) / 32768
    real = np.concatenate([cos, -sin], axis=1)
    imag = np.concatenate([sin, cos], axis=1)
    return split_table(np.stack([real, imag], axis=1).reshape(512, 256))


def regroup_kernel(x_hbm, *refs):
    out_refs, x_ref, sems = refs[:-2], refs[-2], refs[-1]
    copies = []
    for n in range(4):
        rows = pl.ds(1024 * n, 1024)
        copies.append(pltpu.make_async_copy(x_hbm.at[rows], x_ref.at[rows], sems.at[n]))
        copies[n].start()
    for n in range(4):
        copies[n].wait()
        for index, chunk in enumerate(CHUNKS):
            head, rest = out_refs[2 * index], out_refs[2 * index + 1]
            for at, g in enumerate(chunk):
                for c in range(2):
                    lanes = pl.ds(128 * c, 128)

                    def take(first, count):
                        return x_ref[pl.ds(8 * first + 2 * g + c, count, stride=8), :]

                    if n == 0:
                        head[at, 0:128, lanes] = take(0, 128)
                    elif n == 1:
                        head[at, 128:HEAD, lanes] = take(128, HEAD - 128)
                        rest[at, 0 : 256 - HEAD, lanes] = take(HEAD, 256 - HEAD)
                    else:
                        start = 128 * n - HEAD
                        rest[at, start : start + 128, lanes] = take(128 * n, 128)


def regroup(flat):
    shapes = []
    for chunk in CHUNKS:
        shapes.append(jax.ShapeDtypeStruct((len(chunk), HEAD, 256), jnp.float32))
        shapes.append(jax.ShapeDtypeStruct((len(chunk), 512 - HEAD, 256), jnp.float32))
    return pl.pallas_call(
        regroup_kernel,
        out_shape=shapes,
        in_specs=[pl.BlockSpec(memory_space=pltpu.HBM)],
        out_specs=[VMEM] * len(shapes),
        scratch_shapes=[pltpu.VMEM((4096, 128), jnp.float32), pltpu.SemaphoreType.DMA((4,))],
        name="regroup",
        compiler_params=ROOM,
    )(flat)


def place(off_ref, w_ref, at, b):
    here = pl.ds(b * BLOCK, BLOCK)
    tap_at = lax.broadcasted_iota(jnp.int32, (WIN, BLOCK), 0) - off_ref[at, :, here]
    weights = jnp.zeros((WIN, BLOCK), jnp.float32)
    for t in range(TAPS):
        weights = jnp.where(tap_at == t, w_ref[at, pl.ds(t, 1), here], weights)
    return halves(weights)


def place_kernel(off_ref, w_ref, out_ref):
    for at in range(off_ref.shape[0]):
        for b in range(4):
            for n, part in enumerate(place(off_ref, w_ref, at, b)):
                out_ref[pl.ds(WIN * (8 * at + 2 * b + n), WIN), :] = part


def placed(off, weights):
    rows = off.shape[0] * 8 * WIN
    return pl.pallas_call(
        place_kernel,
        out_shape=jax.ShapeDtypeStruct((rows, BLOCK), jnp.bfloat16),
        in_specs=[VMEM, VMEM],
        out_specs=VMEM,
        name="place",
        compiler_params=ROOM,
    )(off, weights)


def remap_kernel(ready, src_ref, off_ref, w_ref, a0, b0, a1, b1, a2, before_ref, out_ref, energy_ref, ext):
    count = a0.shape[0]
    energy = before_ref[...]
    ext[1024 + HEAD :, :] = jnp.zeros((ext.shape[0] - 1024 - HEAD, 256), jnp.float32)
    for at in range(count):
        ext[0:HEAD, :] = a0[at]
        ext[HEAD:512, :] = b0[at]
        ext[512 : 512 + HEAD, :] = a1[at]
        ext[512 + HEAD : 1024, :] = b1[at]
        ext[1024 : 1024 + HEAD, :] = a2[at]
        for b in range(4):
            start = pl.multiple_of(src_ref[at, b] * BLOCK, BLOCK)
            source = ext[pl.ds(start, WIN), :]
            if ready:
                first = WIN * (8 * at + 2 * b)
                w_high = w_ref[pl.ds(first, WIN), :]
                w_low = w_ref[pl.ds(first + WIN, WIN), :]
            else:
                w_high, w_low = place(off_ref, w_ref, at, b)
            s_high, s_low = halves(source)
            result = lax.dot_general(
                jnp.concatenate([w_high, w_high, w_low], axis=0),
                jnp.concatenate([s_high, s_low, s_high], axis=0),
                (((0,), (0,)), ((), ())),
                preferred_element_type=jnp.float32,
            )
            for c in range(2):
                part = result[:, 128 * c : 128 * c + 128].reshape(16, 8, 128)
                out_ref[pl.ds(16 * b, 16), at, c] = part
                energy = energy + jnp.sum(part * part, axis=0)
    energy_ref[...] = energy


def remap(src, off, weights, parts, before):
    count = off.shape[0]
    ready = weights.dtype == jnp.bfloat16
    return pl.pallas_call(
        lambda *refs: remap_kernel(ready, *refs),
        out_shape=[
            jax.ShapeDtypeStruct((64, count, 2, 8, 128), jnp.float32),
            jax.ShapeDtypeStruct((8, 128), jnp.float32),
        ],
        in_specs=[SMEM] + [VMEM] * 8,
        out_specs=[VMEM, VMEM],
        scratch_shapes=[pltpu.VMEM((1024 + WIN, 256), jnp.float32)],
        compiler_params=ROOM,
    )(src, off, weights, *parts, before)


def pack_kernel(x_ref, energy_ref, out_ref):
    total = jnp.full((1, 128), jnp.sum(energy_ref[...]), jnp.float32)
    for a in range(64):
        out_ref[pl.ds(17 * a, 8), :] = x_ref[a, 0, 0]
        out_ref[pl.ds(17 * a + 8, 8), :] = x_ref[a, 0, 1]
        out_ref[pl.ds(17 * a + 16, 1), :] = total


def pack(x, energy):
    return pl.pallas_call(
        pack_kernel,
        out_shape=jax.ShapeDtypeStruct((64 * 17, 128), jnp.float32),
        in_specs=[VMEM, VMEM],
        out_specs=VMEM,
        name="pack",
        compiler_params=ROOM,
    )(x, energy)


def columns(ref, at, stride, rows):
    lanes = []
    for r in rows:
        parts = [ref[pl.ds(16 * at + 8 * c + r, 64, stride=stride), :] for c in range(2)]
        lanes.append(jnp.concatenate(parts, axis=0))
    return halves(jnp.concatenate(lanes, axis=1))


def turned(step, cos, sin):
    lanes = []
    for r in range(step.shape[0] // 128):
        real, imag = step[128 * r : 128 * r + 128, :128], step[128 * r : 128 * r + 128, 128:]
        both = [real * cos - imag * sin, real * sin + imag * cos]
        lanes.append(jnp.concatenate(both, axis=0))
    return halves(jnp.concatenate(lanes, axis=1))


ROWS = ((0,), (0,))
INNER = ((1,), (0,))


def early_kernel(x0, x13, f0h, f0l, f1h, f1l, turn, mh, ml, step_ref, part_ref):
    low = (f0h[...], f0l[...])
    high = (f1h[...], f1l[...])
    step_ref[...] = product(columns(x0, 0, 16, range(8)), low, ROWS)
    for i in range(4):
        rows = (2 * i, 2 * i + 1)
        step = product(columns(x13, 0, 32, rows), low, ROWS)
        step = step + product(columns(x13, 1, 32, rows), high, ROWS)
        data = turned(step, turn[0], turn[1])
        part_ref[:, pl.ds(256 * i, 256)] = product((mh[...], ml[...]), data, INNER)


def early(x0, x13, tables):
    return pl.pallas_call(
        early_kernel,
        out_shape=[
            jax.ShapeDtypeStruct((1024, 256), jnp.float32),
            jax.ShapeDtypeStruct((512, 1024), jnp.float32),
        ],
        in_specs=[VMEM] * 9,
        out_specs=[VMEM, VMEM],
        name="early",
        compiler_params=ROOM,
    )(x0, x13, *tables)


def finish_kernel(*refs):
    sources, out_hbm, held = refs[:8], refs[8], refs[9:17]
    out_ref, load_sems, store_sems = refs[17:]
    x2, fh, fl, turn, mh, ml, step_ref, part_ref = held
    pairs = [(source, here) for source, here in zip(sources[:6], held[:6])]
    for i in range(4):
        rows = pl.ds(256 * i, 256)
        pairs.append((sources[6].at[rows], step_ref.at[rows]))
    for i in range(4):
        lanes = pl.ds(256 * i, 256)
        pairs.append((sources[7].at[:, lanes], part_ref.at[:, lanes]))
    loads = [
        pltpu.make_async_copy(source, here, load_sems.at[n])
        for n, (source, here) in enumerate(pairs)
    ]
    for n in (0, 1, 2, 6, 3, 4, 5, 10, 7, 11, 8, 12, 9, 13):
        loads[n].start()
    for copy in loads[:4]:
        copy.wait()
    energy = jnp.sum(x2[pl.ds(16, 64, stride=17), :], axis=0, keepdims=True)
    scale = lax.rsqrt(energy * (1.0 / (32768.0 * 134217728.0)) + 1e-06)
    stores = []
    for i in range(4):
        pair = (2 * i, 2 * i + 1)
        moved = product(columns(x2, 0, 17, pair), (fh[...], fl[...]), ROWS)
        loads[6 + i].wait()
        data = turned(step_ref[pl.ds(256 * i, 256), :] + moved, turn[0], turn[1])
        if i == 0:
            loads[4].wait()
            loads[5].wait()
        result = product((mh[...], ml[...]), data, INNER)
        loads[10 + i].wait()
        result = result + part_ref[:, pl.ds(256 * i, 256)]
        for at in range(2):
            out_ref[2 * i + at] = result[:, 128 * at : 128 * at + 128] * scale
        both = pl.ds(2 * i, 2)
        stores.append(pltpu.make_async_copy(out_ref.at[both], out_hbm.at[both], store_sems.at[i]))
        stores[i].start()
    for copy in stores:
        copy.wait()


def finish(x2, step, part, tables):
    fh, fl, turn, mh, ml = tables
    operands = (x2, fh, fl, turn, mh, ml, step, part)
    return pl.pallas_call(
        finish_kernel,
        out_shape=jax.ShapeDtypeStruct((8, 512, 128), jnp.float32),
        in_specs=[ANY] * 8,
        out_specs=ANY,
        scratch_shapes=[pltpu.VMEM(x.shape, x.dtype) for x in operands]
        + [
            pltpu.VMEM((8, 512, 128), jnp.float32),
            pltpu.SemaphoreType.DMA((14,)),
            pltpu.SemaphoreType.DMA((4,)),
        ],
        name="finish",
        compiler_params=pltpu.CompilerParams(vmem_limit_bytes=FULL),
    )(*operands)


def steps(spectrum, src_block, offsets, tap_weights):
    position = lax.axis_index("rng")
    size = lax.axis_size("rng")
    down = [(i, i - 1) for i in range(1, size)]
    flat = spectrum.reshape(512, 2, 4, GW).transpose(0, 2, 1, 3).reshape(4096, GW)
    local = regroup(flat)
    src = jnp.clip(src_block - 4 * position, 0, 8)
    off = offsets.reshape(4, 1, 512)
    weights = tap_weights.transpose(1, 0, 2)

    def pull(x):
        return lax.ppermute(x, "rng", down)

    def swap(x):
        return lax.all_to_all(x, AZ, split_axis=0, concat_axis=0, tiled=True)

    energy = jnp.zeros((8, 128), jnp.float32)
    moved = []
    for i, chunk in enumerate(CHUNKS):
        near, far = local[2 * i], local[2 * i + 1]
        near_up = pull(near)
        far_up = pull(far)
        near_up_up = pull(near_up)

        def of_chunk(x):
            return jnp.concatenate([x[g : g + 1] for g in chunk], axis=0)

        off_here, weights_here = of_chunk(off), of_chunk(weights)
        if i == 1:
            weights_here = placed(off_here, weights_here)
        out, energy = remap(
            of_chunk(src), off_here, weights_here, (near, far, near_up, far_up, near_up_up), energy
        )
        moved.append(out)
    got0 = swap(moved[0]).reshape(1024, 128)
    got1 = swap(moved[1]).reshape(2048, 128)
    energy = lax.psum(energy, "rng")
    packed = pack(moved[2], energy).reshape(64, 1, 17 * 128)
    got2 = swap(packed).reshape(1088, 128)
    f0, f1 = first_table(0), first_table(1)
    step, part = early(got0, got1, (*f0, *f1, turn_table(1), *second_table(1)))
    out = finish(got2, step, part, (*f1, turn_table(0), *second_table(0)))
    return out.reshape(8, 256, 2, 128).transpose(0, 2, 1, 3).reshape(8, 2, 32768)


def solution(mesh):
    torus = Mesh(mesh.devices.reshape(mesh.shape["rng"], 8, 4, 2), RNG_AZ)
    placed = (P("rng", None, AZ), P(AZ, "rng"), P(AZ, "rng"), P(None, AZ, "rng"))
    return jax.shard_map(
        steps, mesh=torus, in_specs=placed, out_specs=P(RNG_AZ, None, None), check_vma=False
    )
```

```python
import math

import jax
import jax.numpy as jnp
import numpy as np
from jax import lax
from jax.experimental import pallas as pl
from jax.experimental.pallas import tpu as pltpu
from jax.sharding import Mesh
from jax.sharding import PartitionSpec as P

BLOCK = 128
GW = 128
TAPS = 8
HEAD = 136
WIN = 144
AZ = ("az_0", "az_1", "az_2")
RNG_AZ = ("rng", "az_0", "az_1", "az_2")
CHUNKS = ((0,), (1, 3), (2,))
FULL = 63 << 20
ROOM = pltpu.CompilerParams(vmem_limit_bytes=12 << 20)
VMEM = pl.BlockSpec(memory_space=pltpu.VMEM)
ANY = pl.BlockSpec(memory_space=pl.ANY)
SMEM = pl.BlockSpec(memory_space=pltpu.SMEM)


def halves(x):
    high = x.astype(jnp.bfloat16)
    return high, (x - high.astype(jnp.float32)).astype(jnp.bfloat16)


def product(a, b, contract):
    ((at,), (bt,)) = contract
    left = jnp.concatenate([a[0], a[0], a[1]], axis=at)
    right = jnp.concatenate([b[0], b[1], b[0]], axis=bt)
    return lax.dot_general(left, right, (contract, ((), ())), preferred_element_type=jnp.float32)


def split_table(table):
    high = table.astype(jnp.bfloat16)
    low = (table - high.astype(np.float64)).astype(jnp.bfloat16)
    return high, low


def first_table(upper):
    a = 2 * np.arange(64) + upper
    ang = (a[:, None] * np.arange(128)[None, :] % 128) * (2 * math.pi / 128)
    cos, sin = np.cos(ang), np.sin(ang)
    return split_table(np.block([[cos, sin], [-sin, cos]]))


def turn_table(half):
    ang = (np.arange(128)[:, None] + 128 * half) * np.arange(128)[None, :] * (2 * math.pi / 32768)
    return np.stack([np.cos(ang), np.sin(ang)]).astype(np.float32)


def second_table(half):
    m = np.arange(128) + 128 * half
    ang = (np.arange(256)[:, None] * m[None] % 256) * (2 * math.pi / 256)
    cos, sin = np.cos(ang) / 32768, np.sin(ang) / 32768
    real = np.concatenate([cos, -sin], axis=1)
    imag = np.concatenate([sin, cos], axis=1)
    return split_table(np.stack([real, imag], axis=1).reshape(512, 256))


def regroup_kernel(x_hbm, *refs):
    out_refs, x_ref, sems = refs[:-2], refs[-2], refs[-1]
    copies = []
    for n in range(4):
        rows = pl.ds(1024 * n, 1024)
        copies.append(pltpu.make_async_copy(x_hbm.at[rows], x_ref.at[rows], sems.at[n]))
        copies[n].start()
    for n in range(4):
        copies[n].wait()
        for index, chunk in enumerate(CHUNKS):
            head, rest = out_refs[2 * index], out_refs[2 * index + 1]
            for at, g in enumerate(chunk):
                for c in range(2):
                    lanes = pl.ds(128 * c, 128)

                    def take(first, count):
                        return x_ref[pl.ds(8 * first + 2 * g + c, count, stride=8), :]

                    if n == 0:
                        head[at, 0:128, lanes] = take(0, 128)
                    elif n == 1:
                        head[at, 128:HEAD, lanes] = take(128, HEAD - 128)
                        rest[at, 0 : 256 - HEAD, lanes] = take(HEAD, 256 - HEAD)
                    else:
                        start = 128 * n - HEAD
                        rest[at, start : start + 128, lanes] = take(128 * n, 128)


def regroup(flat):
    shapes = []
    for chunk in CHUNKS:
        shapes.append(jax.ShapeDtypeStruct((len(chunk), HEAD, 256), jnp.float32))
        shapes.append(jax.ShapeDtypeStruct((len(chunk), 512 - HEAD, 256), jnp.float32))
    return pl.pallas_call(
        regroup_kernel,
        out_shape=shapes,
        in_specs=[pl.BlockSpec(memory_space=pltpu.HBM)],
        out_specs=[VMEM] * len(shapes),
        scratch_shapes=[pltpu.VMEM((4096, 128), jnp.float32), pltpu.SemaphoreType.DMA((4,))],
        name="regroup",
        compiler_params=ROOM,
    )(flat)


def place(off_ref, w_ref, at, b):
    here = pl.ds(b * BLOCK, BLOCK)
    tap_at = lax.broadcasted_iota(jnp.int32, (WIN, BLOCK), 0) - off_ref[at, :, here]
    weights = jnp.zeros((WIN, BLOCK), jnp.float32)
    for t in range(TAPS):
        weights = jnp.where(tap_at == t, w_ref[at, pl.ds(t, 1), here], weights)
    return halves(weights)


def place_kernel(off_ref, w_ref, out_ref):
    for at in range(off_ref.shape[0]):
        for b in range(4):
            for n, part in enumerate(place(off_ref, w_ref, at, b)):
                out_ref[pl.ds(WIN * (8 * at + 2 * b + n), WIN), :] = part


def placed(off, weights):
    rows = off.shape[0] * 8 * WIN
    return pl.pallas_call(
        place_kernel,
        out_shape=jax.ShapeDtypeStruct((rows, BLOCK), jnp.bfloat16),
        in_specs=[VMEM, VMEM],
        out_specs=VMEM,
        name="place",
        compiler_params=ROOM,
    )(off, weights)


def remap_kernel(ready, src_ref, off_ref, w_ref, a0, b0, a1, b1, a2, before_ref, out_ref, energy_ref, ext):
    count = a0.shape[0]
    energy = before_ref[...]
    ext[1024 + HEAD :, :] = jnp.zeros((ext.shape[0] - 1024 - HEAD, 256), jnp.float32)
    for at in range(count):
        ext[0:HEAD, :] = a0[at]
        ext[HEAD:512, :] = b0[at]
        ext[512 : 512 + HEAD, :] = a1[at]
        ext[512 + HEAD : 1024, :] = b1[at]
        ext[1024 : 1024 + HEAD, :] = a2[at]
        for b in range(4):
            start = pl.multiple_of(src_ref[at, b] * BLOCK, BLOCK)
            source = ext[pl.ds(start, WIN), :]
            if ready:
                first = WIN * (8 * at + 2 * b)
                w_high = w_ref[pl.ds(first, WIN), :]
                w_low = w_ref[pl.ds(first + WIN, WIN), :]
            else:
                w_high, w_low = place(off_ref, w_ref, at, b)
            s_high, s_low = halves(source)
            result = lax.dot_general(
                jnp.concatenate([w_high, w_high, w_low], axis=0),
                jnp.concatenate([s_high, s_low, s_high], axis=0),
                (((0,), (0,)), ((), ())),
                preferred_element_type=jnp.float32,
            )
            for c in range(2):
                part = result[:, 128 * c : 128 * c + 128].reshape(16, 8, 128)
                out_ref[pl.ds(16 * b, 16), at, c] = part
                energy = energy + jnp.sum(part * part, axis=0)
    energy_ref[...] = energy


def remap(src, off, weights, parts, before):
    count = off.shape[0]
    ready = weights.dtype == jnp.bfloat16
    return pl.pallas_call(
        lambda *refs: remap_kernel(ready, *refs),
        out_shape=[
            jax.ShapeDtypeStruct((64, count, 2, 8, 128), jnp.float32),
            jax.ShapeDtypeStruct((8, 128), jnp.float32),
        ],
        in_specs=[SMEM] + [VMEM] * 8,
        out_specs=[VMEM, VMEM],
        scratch_shapes=[pltpu.VMEM((1024 + WIN, 256), jnp.float32)],
        compiler_params=ROOM,
    )(src, off, weights, *parts, before)


def pack_kernel(x_ref, energy_ref, out_ref):
    total = jnp.full((1, 128), jnp.sum(energy_ref[...]), jnp.float32)
    for a in range(64):
        out_ref[pl.ds(17 * a, 8), :] = x_ref[a, 0, 0]
        out_ref[pl.ds(17 * a + 8, 8), :] = x_ref[a, 0, 1]
        out_ref[pl.ds(17 * a + 16, 1), :] = total


def pack(x, energy):
    return pl.pallas_call(
        pack_kernel,
        out_shape=jax.ShapeDtypeStruct((64 * 17, 128), jnp.float32),
        in_specs=[VMEM, VMEM],
        out_specs=VMEM,
        name="pack",
        compiler_params=ROOM,
    )(x, energy)


def columns(ref, at, stride, rows):
    lanes = []
    for r in rows:
        parts = [ref[pl.ds(16 * at + 8 * c + r, 64, stride=stride), :] for c in range(2)]
        lanes.append(jnp.concatenate(parts, axis=0))
    return halves(jnp.concatenate(lanes, axis=1))


def turned(step, cos, sin):
    lanes = []
    for r in range(step.shape[0] // 128):
        real, imag = step[128 * r : 128 * r + 128, :128], step[128 * r : 128 * r + 128, 128:]
        both = [real * cos - imag * sin, real * sin + imag * cos]
        lanes.append(jnp.concatenate(both, axis=0))
    return halves(jnp.concatenate(lanes, axis=1))


ROWS = ((0,), (0,))
INNER = ((1,), (0,))


def early_kernel(x0, x13, f0h, f0l, f1h, f1l, turn, mh, ml, step_ref, part_ref):
    low = (f0h[...], f0l[...])
    high = (f1h[...], f1l[...])
    step_ref[...] = product(columns(x0, 0, 16, range(8)), low, ROWS)
    for i in range(4):
        rows = (2 * i, 2 * i + 1)
        step = product(columns(x13, 0, 32, rows), low, ROWS)
        step = step + product(columns(x13, 1, 32, rows), high, ROWS)
        data = turned(step, turn[0], turn[1])
        part_ref[:, pl.ds(256 * i, 256)] = product((mh[...], ml[...]), data, INNER)


def early(x0, x13, tables):
    return pl.pallas_call(
        early_kernel,
        out_shape=[
            jax.ShapeDtypeStruct((1024, 256), jnp.float32),
            jax.ShapeDtypeStruct((512, 1024), jnp.float32),
        ],
        in_specs=[VMEM] * 9,
        out_specs=[VMEM, VMEM],
        name="early",
        compiler_params=ROOM,
    )(x0, x13, *tables)


def finish_kernel(*refs):
    sources, out_hbm, held = refs[:8], refs[8], refs[9:17]
    out_ref, load_sems, store_sems = refs[17:]
    x2, fh, fl, turn, mh, ml, step_ref, part_ref = held
    pairs = [(source, here) for source, here in zip(sources[:6], held[:6])]
    for i in range(4):
        rows = pl.ds(256 * i, 256)
        pairs.append((sources[6].at[rows], step_ref.at[rows]))
    for i in range(4):
        lanes = pl.ds(256 * i, 256)
        pairs.append((sources[7].at[:, lanes], part_ref.at[:, lanes]))
    loads = [
        pltpu.make_async_copy(source, here, load_sems.at[n])
        for n, (source, here) in enumerate(pairs)
    ]
    for n in (0, 1, 2, 6, 3, 4, 5, 10, 7, 11, 8, 12, 9, 13):
        loads[n].start()
    for copy in loads[:4]:
        copy.wait()
    energy = jnp.sum(x2[pl.ds(16, 64, stride=17), :], axis=0, keepdims=True)
    scale = lax.rsqrt(energy * (1.0 / (32768.0 * 134217728.0)) + 1e-06)
    stores = []
    for i in range(4):
        pair = (2 * i, 2 * i + 1)
        moved = product(columns(x2, 0, 17, pair), (fh[...], fl[...]), ROWS)
        loads[6 + i].wait()
        data = turned(step_ref[pl.ds(256 * i, 256), :] + moved, turn[0], turn[1])
        if i == 0:
            loads[4].wait()
            loads[5].wait()
        result = product((mh[...], ml[...]), data, INNER)
        loads[10 + i].wait()
        result = result + part_ref[:, pl.ds(256 * i, 256)]
        for at in range(2):
            r = 2 * i + at
            out_ref[r] = result[:, 128 * at : 128 * at + 128] * scale
            stores.append(pltpu.make_async_copy(out_ref.at[r], out_hbm.at[r], store_sems.at[r]))
            stores[r].start()
    for copy in stores:
        copy.wait()


def finish(x2, step, part, tables):
    fh, fl, turn, mh, ml = tables
    operands = (x2, fh, fl, turn, mh, ml, step, part)
    return pl.pallas_call(
        finish_kernel,
        out_shape=jax.ShapeDtypeStruct((8, 512, 128), jnp.float32),
        in_specs=[ANY] * 8,
        out_specs=ANY,
        scratch_shapes=[pltpu.VMEM(x.shape, x.dtype) for x in operands]
        + [
            pltpu.VMEM((8, 512, 128), jnp.float32),
            pltpu.SemaphoreType.DMA((14,)),
            pltpu.SemaphoreType.DMA((8,)),
        ],
        name="finish",
        compiler_params=pltpu.CompilerParams(vmem_limit_bytes=FULL),
    )(*operands)


def steps(spectrum, src_block, offsets, tap_weights):
    position = lax.axis_index("rng")
    size = lax.axis_size("rng")
    down = [(i, i - 1) for i in range(1, size)]
    flat = spectrum.reshape(512, 2, 4, GW).transpose(0, 2, 1, 3).reshape(4096, GW)
    local = regroup(flat)
    src = jnp.clip(src_block - 4 * position, 0, 8)
    off = offsets.reshape(4, 1, 512)
    weights = tap_weights.transpose(1, 0, 2)

    def pull(x):
        return lax.ppermute(x, "rng", down)

    def swap(x):
        return lax.all_to_all(x, AZ, split_axis=0, concat_axis=0, tiled=True)

    energy = jnp.zeros((8, 128), jnp.float32)
    moved = []
    for i, chunk in enumerate(CHUNKS):
        near, far = local[2 * i], local[2 * i + 1]
        near_up = pull(near)
        far_up = pull(far)
        near_up_up = pull(near_up)

        def of_chunk(x):
            return jnp.concatenate([x[g : g + 1] for g in chunk], axis=0)

        off_here, weights_here = of_chunk(off), of_chunk(weights)
        if i == 1:
            weights_here = placed(off_here, weights_here)
        out, energy = remap(
            of_chunk(src), off_here, weights_here, (near, far, near_up, far_up, near_up_up), energy
        )
        moved.append(out)
    got0 = swap(moved[0]).reshape(1024, 128)
    got1 = swap(moved[1]).reshape(2048, 128)
    energy = lax.psum(energy, "rng")
    packed = pack(moved[2], energy).reshape(64, 1, 17 * 128)
    got2 = swap(packed).reshape(1088, 128)
    f0, f1 = first_table(0), first_table(1)
    step, part = early(got0, got1, (*f0, *f1, turn_table(1), *second_table(1)))
    out = finish(got2, step, part, (*f1, turn_table(0), *second_table(0)))
    return out.reshape(8, 256, 2, 128).transpose(0, 2, 1, 3).reshape(8, 2, 32768)


def solution(mesh):
    torus = Mesh(mesh.devices.reshape(mesh.shape["rng"], 8, 4, 2), RNG_AZ)
    placed = (P("rng", None, AZ), P(AZ, "rng"), P(AZ, "rng"), P(None, AZ, "rng"))
    return jax.shard_map(
        steps, mesh=torus, in_specs=placed, out_specs=P(RNG_AZ, None, None), check_vma=False
    )
```
